32 devices in a mesh: pb: 4 (over x, core), dev: 8 (over z, y).
Axes of the slice: x: 2, y: 2, z: 4, core: 2. Of those that a mesh axis runs over, the one named last changes fastest.
Arguments:
- queries: bfloat16 [64, 768], P(('pb', 'dev')), may hold values from -6 to 6
- probes: int32 [64, 16], P(('pb', 'dev')), may hold values from 0 to 1023, all different within a row
- vectors: bfloat16 [16384, 768], P(('pb', 'dev')), may hold values from -0.4375 to 0.4375
- list_ids: int32 [16384], P(('pb', 'dev')), may hold values from 0 to 1023, as said below
Outputs:
- leaders: float32 [64, 100], P(('pb', 'dev'))
The draws below stay inside these ranges and needn't reach their ends.
Inputs may be any that keep to these rules, and one draw needn't show every extreme that they name: `list_ids`: each list id names exactly 16 database vectors. `probes`: each query names 16 different lists.
All inputs are finite; a program needn't handle non-finite values.
Results may differ from the reference program's by a relative error of at most 0.0004.
Values may be sent and summed in bfloat16 or wider, within the bound.
A program may use at most 64 MiB of HBM per device.

```python
import math
import jax
import jax.numpy as jnp
from jax import lax

D = 768
K = 100
NLIST = 1024
NPROBE = 16
QUERIES = 64
VECTORS = 16384


def draw_list_ids(key, part):
    order = jax.random.permutation(key, VECTORS)
    return (order % NLIST).astype(jnp.int32)


def block_levels(own_key, shape, pieces, least, largest):
    factor_of, own = 1.0, jax.random.fold_in(own_key, 6)
    for dim, shards_of in pieces:
        heights = jnp.exp(jax.random.uniform(jax.random.fold_in(own, dim), (shards_of,), jnp.float32, least / len(pieces), largest / len(pieces)))
        factor_of = factor_of * jnp.repeat(heights, shape[dim] // shards_of).reshape([-1 if axis == dim else 1 for axis in range(len(shape))])
    return factor_of


def choose_distinct(key, rows, amount, top, lift):
    ranking = jax.random.permutation(jax.random.fold_in(key, 1), amount)
    boost = ranking
    for power in range(3):
        boost = boost * boost // amount
    boost = boost * lift // amount
    tickets = jax.random.randint(jax.random.fold_in(key, 2), (rows, amount), 0, 4096) + boost
    fixed_rows = jax.random.permutation(jax.random.fold_in(key, 3), rows)[jnp.arange(amount) % rows]
    tickets = jnp.where(jnp.arange(rows)[:, None] == fixed_rows[None, :], 1 << 14, tickets)
    score = tickets * amount + jnp.arange(amount)
    return lax.top_k(score.astype(jnp.int32), top)[1].astype(jnp.int32)


def bell_draw(stream_key, shape, spread, bound, cuts=(), kind=jnp.bfloat16):
    drawn = spread * jax.random.normal(stream_key, shape, jnp.float32)
    if cuts:
        drawn = drawn * block_levels(stream_key, shape, cuts, -0.22, 0.18)
    return jnp.clip(drawn, -bound, bound).astype(kind)


def setup_inputs(seed: int = 0) -> dict:
    arg_keys = jax.random.split(jax.random.key(seed), 5)
    return {
        "queries": bell_draw(arg_keys[0], (QUERIES, D), 1.0, 6.0, ((0, 32),)),
        "probes": choose_distinct(arg_keys[1], QUERIES, NLIST, NPROBE, 128),
        "vectors": bell_draw(arg_keys[2], (VECTORS, D), (D // 4) ** -0.5, 0.4375, ((0, 32),)),
        "list_ids": draw_list_ids(jax.random.fold_in(arg_keys[4], 71), 0),
    }


def reference(queries, probes, vectors, list_ids):
    qblock = math.gcd(QUERIES, 256)
    vblock = math.gcd(VECTORS, 8192)
    slab_rows = vectors.reshape(VECTORS // vblock, vblock, D)
    slab_lists = list_ids.reshape(VECTORS // vblock, vblock)

    def search_block(block_args):
        block_rows, block_probes = block_args
        initial = jnp.full((qblock, K), -1.0e30, jnp.float32)

        def absorb(running, slab):
            slab_part, slab_ids = slab
            products = lax.dot_general(block_rows, slab_part, (((1,), (1,)), ((), ())), preferred_element_type=jnp.float32)
            probed = jnp.any(block_probes[:, :, None] == slab_ids[None, None, :], axis=1)
            filtered = jnp.where(probed, products, jnp.float32(-1.0e30))
            kept, _ = lax.top_k(jnp.concatenate([running, filtered], axis=1), K)
            return kept, None

        kept, _ = lax.scan(absorb, initial, (slab_rows, slab_lists))
        return kept

    leaders = lax.map(search_block, (queries.reshape(QUERIES // qblock, qblock, D), probes.reshape(QUERIES // qblock, qblock, NPROBE)))
    return leaders.reshape(QUERIES, K)
```

```python
import functools

import jax
import jax.numpy as jnp
from jax import lax
from jax.experimental import pallas as pl
from jax.experimental.pallas import tpu as pltpu
from jax.sharding import PartitionSpec as P

K = 100
LIST = 128
SUB = 8
REGS = LIST // SUB
masked_value = -1e30
MESH = pl.DeviceIdType.MESH


def sublane_index():
    return lax.broadcasted_iota(jnp.int32, (SUB, LIST), 0)


def lane_index():
    return lax.broadcasted_iota(jnp.int32, (SUB, LIST), 1)


def sign_where(condition):
    return jnp.where(condition, jnp.float32(-1.0), jnp.float32(1.0))


def register_stage(regs, distance, size):
    out = list(regs)
    for v in range(REGS):
        if v & distance:
            continue
        high, low = jnp.maximum(regs[v], regs[v | distance]), jnp.minimum(regs[v], regs[v | distance])
        if v & size:
            high, low = low, high
        out[v], out[v | distance] = high, low
    return out


def sublane_stage(regs, distance, sub):
    upper = (sub & distance) != 0
    out = []
    for x in regs:
        if 2 * distance == SUB:
            partner = pltpu.roll(x, distance, 0)
        else:
            partner = jnp.where(upper, pltpu.roll(x, distance, 0), pltpu.roll(x, SUB - distance, 0))
        out.append(jnp.where(upper, jnp.minimum(x, partner), jnp.maximum(x, partner)))
    return out


def resort(regs, sub):
    for distance in (4, 2, 1):
        regs = sublane_stage(regs, distance, sub)
    for distance in (8, 4, 2, 1):
        regs = register_stage(regs, distance, 0)
    return regs


def times(regs, sign):
    return [x * sign for x in regs]


def sort_list(regs, sub, sign):
    for size in (2, 4, 8):
        distance = size // 2
        while distance:
            regs = register_stage(regs, distance, size)
            distance //= 2
    now = sign_where((sub & 1) != 0)
    regs = times(regs, now)
    for distance in (8, 4, 2, 1):
        regs = register_stage(regs, distance, 0)
    for step in (1, 2):
        following = sign_where((sub & (2 * step)) != 0)
        regs = times(regs, now * following)
        now = following
        distance = step
        while distance:
            regs = sublane_stage(regs, distance, sub)
            distance //= 2
        for distance in (8, 4, 2, 1):
            regs = register_stage(regs, distance, 0)
    regs = times(regs, now * sign)
    return times(resort(regs, sub), sign)


def split(block):
    return [block[SUB * v : SUB * (v + 1)] for v in range(REGS)]


def join(regs):
    return jnp.concatenate(regs, axis=0)


def larger(left, right):
    return [jnp.maximum(x, y) for x, y in zip(left, right)]


def local_lists(scores, sign):
    sub, lane = sublane_index(), lane_index()
    lists = [split(scores[LIST * i : LIST * (i + 1)]) for i in range(scores.shape[0] // LIST)]
    one, other = jnp.ones((SUB, LIST), jnp.float32), jnp.full((SUB, LIST), -1.0, jnp.float32)
    half_sign = sign_where(lane >= LIST // 2)
    if len(lists) == 1:
        kept = sort_list(lists[0], sub, half_sign)
    else:
        kept = sort_list(lists[0], sub, one)
        for i, item in enumerate(lists[1:]):
            kept = larger(kept, sort_list(item, sub, other))
            final = half_sign if i == len(lists) - 2 else one
            kept = times(resort(times(kept, final), sub), final)
    kept = larger(kept, [pltpu.roll(x, LIST // 2, 1) for x in kept])
    return times(resort(times(kept, sign), sub), sign)


def merge_all(rows, per_device):
    sub, lane = sublane_index(), lane_index()
    pieces = [rows[i : i + LIST] for i in range(0, rows.shape[0], LIST)]
    lanes = pieces[0].shape[0]
    if lanes < LIST:
        pieces = [jnp.concatenate([pieces[0]] * (LIST // lanes), axis=0)]
    blocks = [split(piece.T) for piece in pieces]
    while len(blocks) > 1:
        half = len(blocks) // 2
        merged = [larger(blocks[i], blocks[i + half]) for i in range(half)]
        blocks = []
        for i, regs in enumerate(merged):
            if half == 1:
                sign = sign_where((lane & (lanes // 2)) != 0)
            else:
                sign = jnp.full((SUB, LIST), -1.0 if i >= half // 2 else 1.0, jnp.float32)
            blocks.append(times(resort(times(regs, sign), sub), sign))
    regs = blocks[0]
    stride = lanes // 2
    while stride >= per_device:
        regs = larger(regs, [pltpu.roll(x, LIST - stride, 1) for x in regs])
        stride //= 2
        if stride >= per_device:
            sign = sign_where((lane & stride) != 0)
            regs = times(resort(times(regs, sign), sub), sign)
        else:
            regs = resort(regs, sub)
    return regs


def kernel(
    axes, q_ref, p_ref, v_hbm, id_ref, out_ref,
    v_ref, all_q, all_p, best, arrived, v_sem, own_sem, q_sems, p_sems, s_sems,
):
    (outer, n_outer), (inner, n_inner) = axes
    n = n_outer * n_inner
    me = lax.axis_index(outer) * n_inner + lax.axis_index(inner)
    per_device, depth = q_ref.shape
    rows = v_ref.shape[0]

    def device(k):
        other = lax.rem(me + k, n)
        return other, (other // n_inner, lax.rem(other, n_inner))

    load = pltpu.make_async_copy(v_hbm, v_ref, v_sem)
    load.start()
    own = [
        pltpu.make_async_copy(q_ref, all_q.at[me], own_sem.at[0]),
        pltpu.make_async_copy(p_ref, all_p.at[me], own_sem.at[1]),
    ]
    for copy in own:
        copy.start()

    barrier = pltpu.get_barrier_semaphore()

    @pl.loop(1, n)
    def _(k):
        pl.semaphore_signal(barrier, inc=1, device_id=device(k)[1], device_id_type=MESH)

    pl.semaphore_wait(barrier, n - 1)

    def query_copies(k):
        target = device(k)[1]
        return [
            pltpu.make_async_remote_copy(
                src_ref=src, dst_ref=dst.at[me], send_sem=sems.at[0, k], recv_sem=sems.at[1, k],
                device_id=target, device_id_type=MESH,
            )
            for src, dst, sems in ((q_ref, all_q, q_sems), (p_ref, all_p, p_sems))
        ]

    def score_copy(k):
        other, target = device(k)
        return pltpu.make_async_remote_copy(
            src_ref=best.at[other], dst_ref=arrived.at[me], send_sem=s_sems.at[0, k], recv_sem=s_sems.at[1, k],
            device_id=target, device_id_type=MESH,
        )

    @pl.loop(1, n)
    def _(k):
        for copy in query_copies(k):
            copy.start()

    for copy in own:
        copy.wait()
    load.wait()

    @pl.loop(1, n)
    def _(k):
        for copy in query_copies(k):
            copy.wait()

    lane = lane_index()
    sign = jnp.where(me >= n // 2, jnp.float32(-1.0), jnp.float32(1.0))
    half = LIST // 2
    span = half // per_device
    low_lanes = lax.broadcasted_iota(jnp.int32, (rows // 2, LIST), 1) < half
    ids = jnp.where(
        low_lanes,
        jnp.broadcast_to(id_ref[: rows // 2], (rows // 2, LIST)),
        jnp.broadcast_to(id_ref[rows // 2 :], (rows // 2, LIST)),
    )

    def one_block(b):
        here = pl.ds(b * span, span)
        queries = all_q[here].astype(jnp.float32).reshape(half, depth).astype(jnp.bfloat16)
        queries = jnp.concatenate([queries, queries], axis=0)
        probes = all_p[here].reshape(half, all_p.shape[-1])
        probes = jnp.concatenate([probes, jnp.zeros((half, LIST - probes.shape[1]), jnp.int32)], axis=1)
        probes = jnp.concatenate([probes, probes], axis=0).T
        products = lax.dot_general(
            v_ref[...], queries, (((1,), (1,)), ((), ())), preferred_element_type=jnp.float32
        )
        products = jnp.where(low_lanes, products[: rows // 2], products[rows // 2 :])
        hit = ids == probes[0:1]
        for p in range(1, all_p.shape[-1]):
            hit = hit | (ids == probes[p : p + 1])
        scores = jnp.where(hit, products, jnp.float32(masked_value))
        kept = join(local_lists(scores, sign))
        best[here] = kept.T[:half].reshape(span, per_device, LIST)

    if n == span:
        one_block(0)
    else:
        pl.loop(0, n // span)(one_block)

    @pl.loop(1, n)
    def _(k):
        score_copy(k).start()

    keep = pltpu.make_async_copy(best.at[me], arrived.at[me], own_sem.at[0])
    keep.start()
    keep.wait()

    @pl.loop(1, n)
    def _(k):
        score_copy(k).wait()

    regs = merge_all(arrived[...].reshape(n * per_device, LIST), per_device)
    table = join(regs).reshape(REGS, SUB, LIST)
    ordered = jnp.concatenate([table[:, s] for s in range(SUB)], axis=0)
    out_ref[...] = ordered.T[:per_device, :K]


def solution(mesh):
    axes = tuple(mesh.shape.items())
    n = mesh.size

    def local(queries, probes, vectors, list_ids):
        per_device, depth = queries.shape
        rows = vectors.shape[0]
        return pl.pallas_call(
            functools.partial(kernel, axes),
            out_shape=jax.ShapeDtypeStruct((per_device, K), jnp.float32),
            in_specs=[
                pl.BlockSpec(memory_space=pltpu.VMEM),
                pl.BlockSpec(memory_space=pltpu.VMEM),
                pl.BlockSpec(memory_space=pl.ANY),
                pl.BlockSpec(memory_space=pltpu.VMEM),
            ],
            out_specs=pl.BlockSpec(memory_space=pltpu.VMEM),
            scratch_shapes=[
                pltpu.VMEM((rows, depth), vectors.dtype),
                pltpu.VMEM((n, per_device, depth), queries.dtype),
                pltpu.VMEM((n, per_device, probes.shape[1]), probes.dtype),
                pltpu.VMEM((n, per_device, LIST), jnp.float32),
                pltpu.VMEM((n, per_device, LIST), jnp.float32),
                pltpu.SemaphoreType.DMA,
                pltpu.SemaphoreType.DMA((2,)),
                pltpu.SemaphoreType.DMA((2, n)),
                pltpu.SemaphoreType.DMA((2, n)),
                pltpu.SemaphoreType.DMA((2, n)),
            ],
            compiler_params=pltpu.CompilerParams(collective_id=0, has_side_effects=True),
        )(queries, probes, vectors, list_ids[:, None])

    return jax.shard_map(
        local,
        mesh=mesh,
        in_specs=(
            P(("pb", "dev"), None),
            P(("pb", "dev"), None),
            P(("pb", "dev"), None),
            P(("pb", "dev")),
        ),
        out_specs=P(("pb", "dev"), None),
        check_vma=False,
    )
```

```python
import functools

import jax
import jax.numpy as jnp
from jax import lax
from jax.experimental import pallas as pl
from jax.experimental.pallas import tpu as pltpu
from jax.sharding import PartitionSpec as P

K = 100
LIST = 128
SUB = 8
REGS = LIST // SUB
masked_value = -1e30
MESH = pl.DeviceIdType.MESH


def sublane_index():
    return lax.broadcasted_iota(jnp.int32, (SUB, LIST), 0)


def lane_index():
    return lax.broadcasted_iota(jnp.int32, (SUB, LIST), 1)


def sign_where(condition):
    return jnp.where(condition, jnp.float32(-1.0), jnp.float32(1.0))


def register_stage(regs, distance, size):
    out = list(regs)
    for v in range(REGS):
        if v & distance:
            continue
        high, low = jnp.maximum(regs[v], regs[v | distance]), jnp.minimum(regs[v], regs[v | distance])
        if v & size:
            high, low = low, high
        out[v], out[v | distance] = high, low
    return out


def sublane_stage(regs, distance, sub):
    upper = (sub & distance) != 0
    out = []
    for x in regs:
        if 2 * distance == SUB:
            partner = pltpu.roll(x, distance, 0)
        else:
            partner = jnp.where(upper, pltpu.roll(x, distance, 0), pltpu.roll(x, SUB - distance, 0))
        out.append(jnp.where(upper, jnp.minimum(x, partner), jnp.maximum(x, partner)))
    return out


def resort(regs, sub):
    for distance in (4, 2, 1):
        regs = sublane_stage(regs, distance, sub)
    for distance in (8, 4, 2, 1):
        regs = register_stage(regs, distance, 0)
    return regs


def times(regs, sign):
    return [x * sign for x in regs]


def sort_list(regs, sub, sign):
    for size in (2, 4, 8):
        distance = size // 2
        while distance:
            regs = register_stage(regs, distance, size)
            distance //= 2
    now = sign_where((sub & 1) != 0)
    regs = times(regs, now)
    for distance in (8, 4, 2, 1):
        regs = register_stage(regs, distance, 0)
    for step in (1, 2):
        following = sign_where((sub & (2 * step)) != 0)
        regs = times(regs, now * following)
        now = following
        distance = step
        while distance:
            regs = sublane_stage(regs, distance, sub)
            distance //= 2
        for distance in (8, 4, 2, 1):
            regs = register_stage(regs, distance, 0)
    regs = times(regs, now * sign)
    return times(resort(regs, sub), sign)


def split(block):
    return [block[SUB * v : SUB * (v + 1)] for v in range(REGS)]


def join(regs):
    return jnp.concatenate(regs, axis=0)


def larger(left, right):
    return [jnp.maximum(x, y) for x, y in zip(left, right)]


def local_lists(scores, sign):
    sub, lane = sublane_index(), lane_index()
    lists = [split(scores[LIST * i : LIST * (i + 1)]) for i in range(scores.shape[0] // LIST)]
    one, other = jnp.ones((SUB, LIST), jnp.float32), jnp.full((SUB, LIST), -1.0, jnp.float32)
    half_sign = sign_where(lane >= LIST // 2)
    if len(lists) == 1:
        kept = sort_list(lists[0], sub, half_sign)
    else:
        kept = sort_list(lists[0], sub, one)
        for i, item in enumerate(lists[1:]):
            kept = larger(kept, sort_list(item, sub, other))
            final = half_sign if i == len(lists) - 2 else one
            kept = times(resort(times(kept, final), sub), final)
    kept = larger(kept, [pltpu.roll(x, LIST // 2, 1) for x in kept])
    return times(resort(times(kept, sign), sub), sign)


def merge_all(rows, per_device):
    sub, lane = sublane_index(), lane_index()
    pieces = [rows[i : i + LIST] for i in range(0, rows.shape[0], LIST)]
    lanes = pieces[0].shape[0]
    if lanes < LIST:
        pieces = [jnp.concatenate([pieces[0]] * (LIST // lanes), axis=0)]
    blocks = [split(piece.T) for piece in pieces]
    while len(blocks) > 1:
        half = len(blocks) // 2
        merged = [larger(blocks[i], blocks[i + half]) for i in range(half)]
        blocks = []
        for i, regs in enumerate(merged):
            if half == 1:
                sign = sign_where((lane & (lanes // 2)) != 0)
            else:
                sign = jnp.full((SUB, LIST), -1.0 if i >= half // 2 else 1.0, jnp.float32)
            blocks.append(times(resort(times(regs, sign), sub), sign))
    regs = blocks[0]
    stride = lanes // 2
    while stride >= per_device:
        regs = larger(regs, [pltpu.roll(x, LIST - stride, 1) for x in regs])
        stride //= 2
        if stride >= per_device:
            sign = sign_where((lane & stride) != 0)
            regs = times(resort(times(regs, sign), sub), sign)
        else:
            regs = resort(regs, sub)
    return regs


def kernel(
    axes, q_hbm, p_hbm, v_hbm, id_hbm, arrived,
    q_ref, p_ref, v_ref, id_ref, all_q, all_p, best, load_sems, own_sems, q_sems, p_sems, s_sems,
):
    (outer, n_outer), (inner, n_inner) = axes
    n = n_outer * n_inner
    mine = lax.axis_index(outer), lax.axis_index(inner)
    me = mine[0] * n_inner + mine[1]
    per_device, depth = q_ref.shape
    rows = v_ref.shape[0]

    flips = [[(1 - 2 * ((at // 2**i) % 2)) * 2**i for i in range(n_axis.bit_length() - 1)] for at, n_axis in zip(mine, (n_outer, n_inner))]

    def flipped(at, bits, k):
        for i, flip in enumerate(bits):
            if isinstance(k, int):
                at = at + flip if (k >> i) & 1 else at
            else:
                at = at + flip * ((k // 2**i) % 2)
        return at

    def device(k):
        target = flipped(mine[0], flips[0], k // n_inner), flipped(mine[1], flips[1], k % n_inner)
        return target[0] * n_inner + target[1], target

    def for_peers(body):
        if n <= 64:
            for k in range(n - 1, 0, -1):
                body(k)
        else:
            pl.loop(1, n)(body)

    barrier = pltpu.get_barrier_semaphore()
    for_peers(lambda k: pl.semaphore_signal(barrier, inc=1, device_id=device(k)[1], device_id_type=MESH))
    loads = [
        pltpu.make_async_copy(src, dst, load_sems.at[i])
        for i, (src, dst) in enumerate(((q_hbm, q_ref), (p_hbm, p_ref), (id_hbm, id_ref), (v_hbm, v_ref)))
    ]
    for copy in loads:
        copy.start()
    own = [
        pltpu.make_async_copy(q_ref, all_q.at[me], own_sems.at[0]),
        pltpu.make_async_copy(p_ref, all_p.at[me], own_sems.at[1]),
    ]
    for load, copy in zip(loads[:2], own):
        load.wait()
        copy.start()
    pl.semaphore_wait(barrier, n - 1)

    def remote(src, dst, sems, k, target):
        return pltpu.make_async_remote_copy(
            src_ref=src, dst_ref=dst, send_sem=sems.at[0, k], recv_sem=sems.at[1, k],
            device_id=target, device_id_type=MESH,
        )

    def query_copies(k):
        target = device(k)[1]
        return [remote(q_ref, all_q.at[me], q_sems, k, target), remote(p_ref, all_p.at[me], p_sems, k, target)]

    def score_copy(k):
        other, target = device(k)
        return remote(best.at[other], arrived.at[me], s_sems, k, target)

    def start_queries(k):
        for copy in query_copies(k):
            copy.start()

    def wait_queries(k):
        for copy in query_copies(k):
            copy.wait()

    for_peers(start_queries)
    for copy in own + loads[2:]:
        copy.wait()

    lane = lane_index()
    sign = jnp.where(me >= n // 2, jnp.float32(-1.0), jnp.float32(1.0))
    half = LIST // 2
    span = half // per_device
    low_lanes = lax.broadcasted_iota(jnp.int32, (rows // 2, LIST), 1) < half
    columns = jnp.concatenate(
        [jnp.broadcast_to(id_ref[c : c + 1], (LIST, LIST)).T for c in range(rows // LIST)], axis=0
    )
    ids = jnp.where(low_lanes, columns[: rows // 2], columns[rows // 2 :])
    for_peers(wait_queries)

    def one_block(b):
        here = pl.ds(b * span, span)
        queries = all_q[here].astype(jnp.float32).reshape(half, depth).astype(jnp.bfloat16)
        queries = jnp.concatenate([queries, queries], axis=0)
        probes = all_p[here].reshape(half, all_p.shape[-1])
        probes = jnp.concatenate([probes, jnp.zeros((half, LIST - probes.shape[1]), jnp.int32)], axis=1)
        probes = jnp.concatenate([probes, probes], axis=0).T
        products = lax.dot_general(
            v_ref[...], queries, (((1,), (1,)), ((), ())), preferred_element_type=jnp.float32
        )
        products = jnp.where(low_lanes, products[: rows // 2], products[rows // 2 :])
        hit = ids == probes[0:1]
        for p in range(1, all_p.shape[-1]):
            hit = hit | (ids == probes[p : p + 1])
        scores = jnp.where(hit, products, jnp.float32(masked_value))
        kept = join(local_lists(scores, sign))
        best[here] = kept.T[:half].reshape(span, per_device, LIST)

    if n == span:
        one_block(0)
    else:
        pl.loop(0, n // span)(one_block)

    for_peers(lambda k: score_copy(k).start())
    keep = pltpu.make_async_copy(best.at[me], arrived.at[me], own_sems.at[0])
    keep.start()
    for_peers(lambda k: score_copy(k).wait())
    keep.wait()


def finish(arrived, out_ref):
    n, per_device, _ = arrived.shape
    regs = merge_all(arrived[...].reshape(n * per_device, LIST), per_device)
    table = join(regs).reshape(REGS, SUB, LIST)
    ordered = jnp.concatenate([table[:, s] for s in range(SUB)], axis=0)
    out_ref[...] = ordered.T[:per_device, :K]


def solution(mesh):
    axes = tuple(mesh.shape.items())
    n = mesh.size

    def local(queries, probes, vectors, list_ids):
        per_device, depth = queries.shape
        rows = vectors.shape[0]
        arrived = pl.pallas_call(
            functools.partial(kernel, axes),
            out_shape=jax.ShapeDtypeStruct((n, per_device, LIST), jnp.float32),
            in_specs=[pl.BlockSpec(memory_space=pl.ANY)] * 4,
            out_specs=pl.BlockSpec(memory_space=pl.ANY),
            scratch_shapes=[
                pltpu.VMEM((per_device, depth), queries.dtype),
                pltpu.VMEM(probes.shape, probes.dtype),
                pltpu.VMEM((rows, depth), vectors.dtype),
                pltpu.VMEM((rows // LIST, LIST), list_ids.dtype),
                pltpu.VMEM((n, per_device, depth), queries.dtype),
                pltpu.VMEM((n, per_device, probes.shape[1]), probes.dtype),
                pltpu.VMEM((n, per_device, LIST), jnp.float32),
                pltpu.SemaphoreType.DMA((4,)),
                pltpu.SemaphoreType.DMA((2,)),
                pltpu.SemaphoreType.DMA((2, n)),
                pltpu.SemaphoreType.DMA((2, n)),
                pltpu.SemaphoreType.DMA((2, n)),
            ],
            compiler_params=pltpu.CompilerParams(collective_id=0, has_side_effects=True),
        )(queries, probes, vectors, list_ids.reshape(rows // LIST, LIST))
        return pl.pallas_call(
            finish,
            out_shape=jax.ShapeDtypeStruct((per_device, K), jnp.float32),
            in_specs=[pl.BlockSpec(memory_space=pltpu.VMEM)],
            out_specs=pl.BlockSpec(memory_space=pltpu.VMEM),
        )(arrived)

    return jax.shard_map(
        local,
        mesh=mesh,
        in_specs=(
            P(("pb", "dev"), None),
            P(("pb", "dev"), None),
            P(("pb", "dev"), None),
            P(("pb", "dev")),
        ),
        out_specs=P(("pb", "dev"), None),
        check_vma=False,
    )
```

```python
import functools

import jax
import jax.numpy as jnp
from jax import lax
from jax.experimental import pallas as pl
from jax.experimental.pallas import tpu as pltpu
from jax.sharding import PartitionSpec as P

K = 100
LIST = 128
SUB = 8
REGS = LIST // SUB
masked_value = -1e30
MESH = pl.DeviceIdType.MESH


def sublane_index():
    return lax.broadcasted_iota(jnp.int32, (SUB, LIST), 0)


def lane_index():
    return lax.broadcasted_iota(jnp.int32, (SUB, LIST), 1)


def sign_where(condition):
    return jnp.where(condition, jnp.float32(-1.0), jnp.float32(1.0))


def register_stage(regs, distance, size):
    out = list(regs)
    for v in range(REGS):
        if v & distance:
            continue
        high, low = jnp.maximum(regs[v], regs[v | distance]), jnp.minimum(regs[v], regs[v | distance])
        if v & size:
            high, low = low, high
        out[v], out[v | distance] = high, low
    return out


def sublane_stage(regs, distance, sub):
    upper = (sub & distance) != 0
    out = []
    for x in regs:
        if 2 * distance == SUB:
            partner = pltpu.roll(x, distance, 0)
        else:
            partner = jnp.where(upper, pltpu.roll(x, distance, 0), pltpu.roll(x, SUB - distance, 0))
        out.append(jnp.where(upper, jnp.minimum(x, partner), jnp.maximum(x, partner)))
    return out


def resort(regs, sub):
    for distance in (4, 2, 1):
        regs = sublane_stage(regs, distance, sub)
    for distance in (8, 4, 2, 1):
        regs = register_stage(regs, distance, 0)
    return regs


def times(regs, sign):
    return [x * sign for x in regs]


def sort_list(regs, sub, sign):
    for size in (2, 4, 8):
        distance = size // 2
        while distance:
            regs = register_stage(regs, distance, size)
            distance //= 2
    now = sign_where((sub & 1) != 0)
    regs = times(regs, now)
    for distance in (8, 4, 2, 1):
        regs = register_stage(regs, distance, 0)
    for step in (1, 2):
        following = sign_where((sub & (2 * step)) != 0)
        regs = times(regs, now * following)
        now = following
        distance = step
        while distance:
            regs = sublane_stage(regs, distance, sub)
            distance //= 2
        for distance in (8, 4, 2, 1):
            regs = register_stage(regs, distance, 0)
    regs = times(regs, now * sign)
    return times(resort(regs, sub), sign)


def split(block):
    return [block[SUB * v : SUB * (v + 1)] for v in range(REGS)]


def join(regs):
    return jnp.concatenate(regs, axis=0)


def larger(left, right):
    return [jnp.maximum(x, y) for x, y in zip(left, right)]


def local_lists(scores, sign):
    sub, lane = sublane_index(), lane_index()
    lists = [split(scores[LIST * i : LIST * (i + 1)]) for i in range(scores.shape[0] // LIST)]
    one, other = jnp.ones((SUB, LIST), jnp.float32), jnp.full((SUB, LIST), -1.0, jnp.float32)
    half_sign = sign_where(lane >= LIST // 2)
    if len(lists) == 1:
        kept = sort_list(lists[0], sub, half_sign)
    else:
        kept = sort_list(lists[0], sub, one)
        for i, item in enumerate(lists[1:]):
            kept = larger(kept, sort_list(item, sub, other))
            final = half_sign if i == len(lists) - 2 else one
            kept = times(resort(times(kept, final), sub), final)
    kept = larger(kept, [pltpu.roll(x, LIST // 2, 1) for x in kept])
    return times(resort(times(kept, sign), sub), sign)


def merge_all(rows, per_device):
    sub, lane = sublane_index(), lane_index()
    pieces = [rows[i : i + LIST] for i in range(0, rows.shape[0], LIST)]
    lanes = pieces[0].shape[0]
    if lanes < LIST:
        pieces = [jnp.concatenate([pieces[0]] * (LIST // lanes), axis=0)]
    blocks = [split(piece.T) for piece in pieces]
    while len(blocks) > 1:
        half = len(blocks) // 2
        merged = [larger(blocks[i], blocks[i + half]) for i in range(half)]
        blocks = []
        for i, regs in enumerate(merged):
            if half == 1:
                sign = sign_where((lane & (lanes // 2)) != 0)
            else:
                sign = jnp.full((SUB, LIST), -1.0 if i >= half // 2 else 1.0, jnp.float32)
            blocks.append(times(resort(times(regs, sign), sub), sign))
    regs = blocks[0]
    stride = lanes // 2
    while stride >= per_device:
        regs = larger(regs, [pltpu.roll(x, LIST - stride, 1) for x in regs])
        stride //= 2
        if stride >= per_device:
            sign = sign_where((lane & stride) != 0)
            regs = times(resort(times(regs, sign), sub), sign)
        else:
            regs = resort(regs, sub)
    return regs


def kernel(
    axes, q_hbm, p_hbm, v_hbm, id_hbm, arrived,
    packed, p_ref, v_ref, id_ref, gathered, best, load_sems, own_sem, q_sems, s_sems,
):
    (outer, n_outer), (inner, n_inner) = axes
    n = n_outer * n_inner
    mine = lax.axis_index(outer), lax.axis_index(inner)
    me = mine[0] * n_inner + mine[1]
    per_device, depth = q_hbm.shape
    n_probes = p_ref.shape[1]
    rows = v_ref.shape[0]

    flips = [[(1 - 2 * ((at // 2**i) % 2)) * 2**i for i in range(n_axis.bit_length() - 1)] for at, n_axis in zip(mine, (n_outer, n_inner))]

    def flipped(at, bits, k):
        for i, flip in enumerate(bits):
            if isinstance(k, int):
                at = at + flip if (k >> i) & 1 else at
            else:
                at = at + flip * ((k // 2**i) % 2)
        return at

    def device(k):
        target = flipped(mine[0], flips[0], k // n_inner), flipped(mine[1], flips[1], k % n_inner)
        return target[0] * n_inner + target[1], target

    def reach(k):
        far, near = divmod(k, n_inner)
        return near // 2 + near % 2 + (far // 2).bit_count() + 0.25 * (far % 2), k

    def for_peers(body):
        if n <= 64:
            for k in sorted(range(1, n), key=reach, reverse=True):
                body(k)
        else:
            pl.loop(1, n)(body)

    barrier = pltpu.get_barrier_semaphore()
    for_peers(lambda k: pl.semaphore_signal(barrier, inc=1, device_id=device(k)[1], device_id_type=MESH))
    loads = [
        pltpu.make_async_copy(src, dst, load_sems.at[i])
        for i, (src, dst) in enumerate(((p_hbm, p_ref), (q_hbm, packed.at[:, :depth]), (id_hbm, id_ref), (v_hbm, v_ref)))
    ]
    for copy in loads:
        copy.start()
    loads[0].wait()
    digits = jnp.concatenate([p_ref[...] // 256, p_ref[...] % 256], axis=1).astype(jnp.float32)
    digits = jnp.concatenate([digits, jnp.zeros((per_device, LIST - 2 * n_probes), jnp.float32)], axis=1)
    packed[:, depth:] = digits.astype(packed.dtype)
    loads[1].wait()
    own = pltpu.make_async_copy(packed, gathered.at[me], own_sem)
    own.start()
    pl.semaphore_wait(barrier, n - 1)

    def remote(src, dst, sems, k, target):
        return pltpu.make_async_remote_copy(
            src_ref=src, dst_ref=dst, send_sem=sems.at[0, k], recv_sem=sems.at[1, k],
            device_id=target, device_id_type=MESH,
        )

    def query_copy(k):
        return remote(packed, gathered.at[me], q_sems, k, device(k)[1])

    def score_copy(k):
        other, target = device(k)
        return remote(best.at[other], arrived.at[me], s_sems, k, target)

    for_peers(lambda k: query_copy(k).start())
    for copy in [own] + loads[2:]:
        copy.wait()

    lane = lane_index()
    sign = jnp.where(me >= n // 2, jnp.float32(-1.0), jnp.float32(1.0))
    half = LIST // 2
    span = half // per_device
    low_lanes = lax.broadcasted_iota(jnp.int32, (rows // 2, LIST), 1) < half
    columns = jnp.concatenate(
        [jnp.broadcast_to(id_ref[c : c + 1], (LIST, LIST)).T for c in range(rows // LIST)], axis=0
    )
    ids = jnp.where(low_lanes, columns[: rows // 2], columns[rows // 2 :]).astype(jnp.float32)
    for_peers(lambda k: query_copy(k).wait())

    def one_block(b):
        here = pl.ds(b * span, span)
        together = gathered[here].astype(jnp.float32).reshape(half, depth + LIST)
        queries = together[:, :depth].astype(jnp.bfloat16)
        queries = jnp.concatenate([queries, queries], axis=0)
        digits = together[:, depth:]
        digits = jnp.concatenate([digits, digits], axis=0).T
        probes = digits[:n_probes] * 256.0 + digits[n_probes : 2 * n_probes]
        products = lax.dot_general(
            v_ref[...], queries, (((1,), (1,)), ((), ())), preferred_element_type=jnp.float32
        )
        products = jnp.where(low_lanes, products[: rows // 2], products[rows // 2 :])
        hit = ids == probes[0:1]
        for p in range(1, n_probes):
            hit = hit | (ids == probes[p : p + 1])
        scores = jnp.where(hit, products, jnp.float32(masked_value))
        kept = join(local_lists(scores, sign))
        best[here] = kept.T[:half].reshape(span, per_device, LIST)

    if n == span:
        one_block(0)
    else:
        pl.loop(0, n // span)(one_block)

    for_peers(lambda k: score_copy(k).start())
    keep = pltpu.make_async_copy(best.at[me], arrived.at[me], own_sem)
    keep.start()
    for_peers(lambda k: score_copy(k).wait())
    keep.wait()


def finish(arrived, out_ref):
    n, per_device, _ = arrived.shape
    regs = merge_all(arrived[...].reshape(n * per_device, LIST), per_device)
    table = join(regs).reshape(REGS, SUB, LIST)
    ordered = jnp.concatenate([table[:, s] for s in range(SUB)], axis=0)
    out_ref[...] = ordered.T[:per_device, :K]


def solution(mesh):
    axes = tuple(mesh.shape.items())
    n = mesh.size

    def local(queries, probes, vectors, list_ids):
        per_device, depth = queries.shape
        rows = vectors.shape[0]
        arrived = pl.pallas_call(
            functools.partial(kernel, axes),
            out_shape=pltpu.VMEM((n, per_device, LIST), jnp.float32),
            in_specs=[pl.BlockSpec(memory_space=pl.ANY)] * 4,
            out_specs=pl.BlockSpec(memory_space=pltpu.VMEM),
            scratch_shapes=[
                pltpu.VMEM((per_device, depth + LIST), queries.dtype),
                pltpu.VMEM(probes.shape, probes.dtype),
                pltpu.VMEM((rows, depth), vectors.dtype),
                pltpu.VMEM((rows // LIST, LIST), list_ids.dtype),
                pltpu.VMEM((n, per_device, depth + LIST), queries.dtype),
                pltpu.VMEM((n, per_device, LIST), jnp.float32),
                pltpu.SemaphoreType.DMA((4,)),
                pltpu.SemaphoreType.DMA,
                pltpu.SemaphoreType.DMA((2, n)),
                pltpu.SemaphoreType.DMA((2, n)),
            ],
            compiler_params=pltpu.CompilerParams(collective_id=0, has_side_effects=True),
        )(queries, probes, vectors, list_ids.reshape(rows // LIST, LIST))
        return pl.pallas_call(
            finish,
            out_shape=jax.ShapeDtypeStruct((per_device, K), jnp.float32),
            in_specs=[pl.BlockSpec(memory_space=pltpu.VMEM)],
            compiler_params=pltpu.CompilerParams(vmem_limit_bytes=4 << 20),
            out_specs=pl.BlockSpec(memory_space=pltpu.VMEM),
        )(arrived)

    return jax.shard_map(
        local,
        mesh=mesh,
        in_specs=(
            P(("pb", "dev"), None),
            P(("pb", "dev"), None),
            P(("pb", "dev"), None),
            P(("pb", "dev")),
        ),
        out_specs=P(("pb", "dev"), None),
        check_vma=False,
    )
```

```python
import functools

import jax
import jax.numpy as jnp
from jax import lax
from jax.experimental import pallas as pl
from jax.experimental.pallas import tpu as pltpu
from jax.sharding import PartitionSpec as P

K = 100
LIST = 128
SUB = 8
REGS = LIST // SUB
masked_value = -1e30
MESH = pl.DeviceIdType.MESH


def sublane_index():
    return lax.broadcasted_iota(jnp.int32, (SUB, LIST), 0)


def lane_index():
    return lax.broadcasted_iota(jnp.int32, (SUB, LIST), 1)


def sign_where(condition):
    return jnp.where(condition, jnp.float32(-1.0), jnp.float32(1.0))


def register_stage(regs, distance, size):
    out = list(regs)
    for v in range(REGS):
        if v & distance:
            continue
        high, low = jnp.maximum(regs[v], regs[v | distance]), jnp.minimum(regs[v], regs[v | distance])
        if v & size:
            high, low = low, high
        out[v], out[v | distance] = high, low
    return out


def sublane_stage(regs, distance, sub):
    upper = (sub & distance) != 0
    out = []
    for x in regs:
        if 2 * distance == SUB:
            partner = pltpu.roll(x, distance, 0)
        else:
            partner = jnp.where(upper, pltpu.roll(x, distance, 0), pltpu.roll(x, SUB - distance, 0))
        out.append(jnp.where(upper, jnp.minimum(x, partner), jnp.maximum(x, partner)))
    return out


def resort(regs, sub):
    for distance in (4, 2, 1):
        regs = sublane_stage(regs, distance, sub)
    for distance in (8, 4, 2, 1):
        regs = register_stage(regs, distance, 0)
    return regs


def times(regs, sign):
    return [x * sign for x in regs]


def sort_list(regs, sub, sign):
    for size in (2, 4, 8):
        distance = size // 2
        while distance:
            regs = register_stage(regs, distance, size)
            distance //= 2
    now = sign_where((sub & 1) != 0)
    regs = times(regs, now)
    for distance in (8, 4, 2, 1):
        regs = register_stage(regs, distance, 0)
    for step in (1, 2):
        following = sign_where((sub & (2 * step)) != 0)
        regs = times(regs, now * following)
        now = following
        distance = step
        while distance:
            regs = sublane_stage(regs, distance, sub)
            distance //= 2
        for distance in (8, 4, 2, 1):
            regs = register_stage(regs, distance, 0)
    regs = times(regs, now * sign)
    return times(resort(regs, sub), sign)


def split(block):
    return [block[SUB * v : SUB * (v + 1)] for v in range(REGS)]


def join(regs):
    return jnp.concatenate(regs, axis=0)


def larger(left, right):
    return [jnp.maximum(x, y) for x, y in zip(left, right)]


def local_lists(scores, sign):
    sub, lane = sublane_index(), lane_index()
    lists = [split(scores[LIST * i : LIST * (i + 1)]) for i in range(scores.shape[0] // LIST)]
    one, other = jnp.ones((SUB, LIST), jnp.float32), jnp.full((SUB, LIST), -1.0, jnp.float32)
    half_sign = sign_where(lane >= LIST // 2)
    if len(lists) == 1:
        kept = sort_list(lists[0], sub, half_sign)
    else:
        kept = sort_list(lists[0], sub, one)
        for i, item in enumerate(lists[1:]):
            kept = larger(kept, sort_list(item, sub, other))
            final = half_sign if i == len(lists) - 2 else one
            kept = times(resort(times(kept, final), sub), final)
    kept = larger(kept, [pltpu.roll(x, LIST // 2, 1) for x in kept])
    return times(resort(times(kept, sign), sub), sign)


def merge_all(rows, per_device):
    sub, lane = sublane_index(), lane_index()
    pieces = [rows[i : i + LIST] for i in range(0, rows.shape[0], LIST)]
    lanes = pieces[0].shape[0]
    if lanes < LIST:
        pieces = [jnp.concatenate([pieces[0]] * (LIST // lanes), axis=0)]
    blocks = [split(piece.T) for piece in pieces]
    while len(blocks) > 1:
        half = len(blocks) // 2
        merged = [larger(blocks[i], blocks[i + half]) for i in range(half)]
        blocks = []
        for i, regs in enumerate(merged):
            if half == 1:
                sign = sign_where((lane & (lanes // 2)) != 0)
            else:
                sign = jnp.full((SUB, LIST), -1.0 if i >= half // 2 else 1.0, jnp.float32)
            blocks.append(times(resort(times(regs, sign), sub), sign))
    regs = blocks[0]
    stride = lanes // 2
    while stride >= per_device:
        regs = larger(regs, [pltpu.roll(x, LIST - stride, 1) for x in regs])
        stride //= 2
        if stride >= per_device:
            sign = sign_where((lane & stride) != 0)
            regs = times(resort(times(regs, sign), sub), sign)
        else:
            regs = resort(regs, sub)
    return regs


def kernel(
    axes, q_hbm, p_hbm, v_hbm, id_hbm, arrived,
    packed, p_ref, v_ref, id_ref, gathered, best, load_sems, own_sem, q_sems, s_sems,
):
    (outer, n_outer), (inner, n_inner) = axes
    n = n_outer * n_inner
    mine = lax.axis_index(outer), lax.axis_index(inner)
    me = mine[0] * n_inner + mine[1]
    per_device, depth = q_hbm.shape
    n_probes = p_ref.shape[1]
    rows = v_ref.shape[0]

    flips = [[(1 - 2 * ((at // 2**i) % 2)) * 2**i for i in range(n_axis.bit_length() - 1)] for at, n_axis in zip(mine, (n_outer, n_inner))]

    def flipped(at, bits, k):
        for i, flip in enumerate(bits):
            if isinstance(k, int):
                at = at + flip if (k >> i) & 1 else at
            else:
                at = at + flip * ((k // 2**i) % 2)
        return at

    def device(k):
        target = flipped(mine[0], flips[0], k // n_inner), flipped(mine[1], flips[1], k % n_inner)
        return target[0] * n_inner + target[1], target

    def reach(k):
        far, near = divmod(k, n_inner)
        return near // 2 + near % 2 + (far // 2).bit_count() + 0.25 * (far % 2), k

    def for_peers(body):
        if n <= 64:
            for k in sorted(range(1, n), key=reach, reverse=True):
                body(k)
        else:
            pl.loop(1, n)(body)

    barrier = pltpu.get_barrier_semaphore()
    for_peers(lambda k: pl.semaphore_signal(barrier, inc=1, device_id=device(k)[1], device_id_type=MESH))
    loads = [
        pltpu.make_async_copy(src, dst, load_sems.at[i])
        for i, (src, dst) in enumerate(((p_hbm, p_ref), (q_hbm, packed.at[:, :depth]), (id_hbm, id_ref), (v_hbm, v_ref)))
    ]
    for copy in loads:
        copy.start()
    loads[0].wait()
    digits = jnp.concatenate([p_ref[...] // 256, p_ref[...] % 256], axis=1).astype(jnp.float32)
    digits = jnp.concatenate([digits, jnp.zeros((per_device, LIST - 2 * n_probes), jnp.float32)], axis=1)
    packed[:, depth:] = digits.astype(packed.dtype)
    loads[1].wait()
    own = pltpu.make_async_copy(packed, gathered.at[me], own_sem)
    own.start()
    pl.semaphore_wait(barrier, n - 1)

    def remote(src, dst, sems, k, target):
        return pltpu.make_async_remote_copy(
            src_ref=src, dst_ref=dst, send_sem=sems.at[0, k], recv_sem=sems.at[1, k],
            device_id=target, device_id_type=MESH,
        )

    def query_copy(k):
        return remote(packed, gathered.at[me], q_sems, k, device(k)[1])

    def score_copy(k):
        other, target = device(k)
        return remote(best.at[other], arrived.at[me], s_sems, k, target)

    for_peers(lambda k: query_copy(k).start())
    for copy in [own] + loads[2:]:
        copy.wait()

    lane = lane_index()
    sign = jnp.where(me >= n // 2, jnp.float32(-1.0), jnp.float32(1.0))
    half = LIST // 2
    span = half // per_device
    low_lanes = lax.broadcasted_iota(jnp.int32, (rows // 2, LIST), 1) < half
    columns = jnp.concatenate(
        [jnp.broadcast_to(id_ref[c : c + 1], (LIST, LIST)).T for c in range(rows // LIST)], axis=0
    )
    ids = jnp.where(low_lanes, columns[: rows // 2], columns[rows // 2 :]).astype(jnp.float32)
    for_peers(lambda k: query_copy(k).wait_recv())

    def one_block(b):
        here = pl.ds(b * span, span)
        together = gathered[here].reshape(half, depth + LIST)
        queries = together[:, :depth]
        queries = jnp.concatenate([queries, queries], axis=0)
        digits = together[:, depth:].astype(jnp.float32)
        digits = jnp.concatenate([digits, digits], axis=0).T
        probes = digits[:n_probes] * 256.0 + digits[n_probes : 2 * n_probes]
        products = lax.dot_general(
            v_ref[...], queries, (((1,), (1,)), ((), ())), preferred_element_type=jnp.float32
        )
        products = jnp.where(low_lanes, products[: rows // 2], products[rows // 2 :])
        hit = ids == probes[0:1]
        for p in range(1, n_probes):
            hit = hit | (ids == probes[p : p + 1])
        scores = jnp.where(hit, products, jnp.float32(masked_value))
        kept = join(local_lists(scores, sign))
        best[here] = kept.T[:half].reshape(span, per_device, LIST)

    if n == span:
        one_block(0)
    else:
        pl.loop(0, n // span)(one_block)

    for_peers(lambda k: score_copy(k).start())
    keep = pltpu.make_async_copy(best.at[me], arrived.at[me], own_sem)
    keep.start()
    for_peers(lambda k: query_copy(k).wait_send())
    for_peers(lambda k: score_copy(k).wait_send())
    keep.wait()
    for_peers(lambda k: score_copy(k).wait_recv())


def finish(arrived, out_ref):
    n, per_device, _ = arrived.shape
    regs = merge_all(arrived[...].reshape(n * per_device, LIST), per_device)
    table = join(regs).reshape(REGS, SUB, LIST)
    ordered = jnp.concatenate([table[:, s] for s in range(SUB)], axis=0)
    out_ref[...] = ordered.T[:per_device, :K]


def solution(mesh):
    axes = tuple(mesh.shape.items())
    n = mesh.size

    def local(queries, probes, vectors, list_ids):
        per_device, depth = queries.shape
        rows = vectors.shape[0]
        arrived = pl.pallas_call(
            functools.partial(kernel, axes),
            out_shape=pltpu.VMEM((n, per_device, LIST), jnp.float32),
            in_specs=[pl.BlockSpec(memory_space=pl.ANY)] * 4,
            out_specs=pl.BlockSpec(memory_space=pltpu.VMEM),
            scratch_shapes=[
                pltpu.VMEM((per_device, depth + LIST), queries.dtype),
                pltpu.VMEM(probes.shape, probes.dtype),
                pltpu.VMEM((rows, depth), vectors.dtype),
                pltpu.VMEM((rows // LIST, LIST), list_ids.dtype),
                pltpu.VMEM((n, per_device, depth + LIST), queries.dtype),
                pltpu.VMEM((n, per_device, LIST), jnp.float32),
                pltpu.SemaphoreType.DMA((4,)),
                pltpu.SemaphoreType.DMA,
                pltpu.SemaphoreType.DMA((2, n)),
                pltpu.SemaphoreType.DMA((2, n)),
            ],
            compiler_params=pltpu.CompilerParams(collective_id=0, has_side_effects=True),
        )(queries, probes, vectors, list_ids.reshape(rows // LIST, LIST))
        return pl.pallas_call(
            finish,
            out_shape=jax.ShapeDtypeStruct((per_device, K), jnp.float32),
            in_specs=[pl.BlockSpec(memory_space=pltpu.VMEM)],
            compiler_params=pltpu.CompilerParams(vmem_limit_bytes=4 << 20),
            out_specs=pl.BlockSpec(memory_space=pltpu.VMEM),
        )(arrived)

    return jax.shard_map(
        local,
        mesh=mesh,
        in_specs=(
            P(("pb", "dev"), None),
            P(("pb", "dev"), None),
            P(("pb", "dev"), None),
            P(("pb", "dev")),
        ),
        out_specs=P(("pb", "dev"), None),
        check_vma=False,
    )
```
